32 devices in a mesh: row: 4 (over z), col: 8 (over y, x, core).
Axes of the slice: x: 2, y: 2, z: 4, core: 2. Of those that a mesh axis runs over, the one named last changes fastest.
Arguments:
- node_latent: bfloat16 [32768, 128], P(('row', 'col')), may hold values from -6 to 6
- edge_latent: bfloat16 [131072, 128], P(('row', 'col')), may hold values from -6 to 6
- senders: int32 [131072], P(('row', 'col')), may hold values from 0 to 1535
- receivers: int32 [131072], P(('row', 'col')), may hold values from 0 to 1023
- send_index: int32 [32, 4, 128], P(('row', 'col')), may hold values from 0 to 1023
- context_table: bfloat16 [256, 128], P(('row', 'col')), may hold values from -6 to 6
- region: int32 [32768], P(('row', 'col')), may hold values from 0 to 255
- edge_w1: bfloat16 [2, 384, 128], replicated, may hold values from -0.3125 to 0.3125
- edge_w2: bfloat16 [2, 128, 128], replicated, may hold values from -0.5 to 0.5
- edge_bias: float32 [2, 3, 128], replicated, may hold values from -3 to 3
- edge_gain: float32 [2, 128], replicated, may hold values from 0.25 to 1.75
- node_w1: bfloat16 [2, 384, 128], replicated, may hold values from -0.3125 to 0.3125
- node_wg: bfloat16 [2, 128, 128], replicated, may hold values from -0.5 to 0.5
- node_w2: bfloat16 [2, 128, 128], replicated, may hold values from -0.5 to 0.5
- node_bias: float32 [2, 3, 128], replicated, may hold values from -3 to 3
- node_gain: float32 [2, 128], replicated, may hold values from 0.25 to 1.75
Outputs:
- node_out: bfloat16 [32768, 128], P(('row', 'col'))
- edge_out: bfloat16 [131072, 128], P(('row', 'col'))
The draws below stay inside these ranges and needn't reach their ends.
Inputs may be any that keep to these rules, and one draw needn't show every extreme that they name: senders index the extended table of the edge's own partition: below 1024 its own nodes, then the four received blocks of 128 rows in the order above, below, left, right. receivers are nodes of the edge's own partition. `send_index`: rows of the sending partition's own nodes; repeats may occur.
All inputs are finite; a program needn't handle non-finite values.
Results may differ from the reference program's by a relative error of at most 0.0085.
Values may be sent and summed in bfloat16 or wider, within the bound.
A program may use at most 64 MiB of HBM per device.

```python
import math
import jax
import jax.numpy as jnp
from jax import lax

LATENT = 128
NODES_DEV = 1024
BOUNDARY = 128
LAYERS = 2
EDGES_DEV = 4096
EXTENDED = 1536
PARTS_SIZE = 32
NODES = 32768
EDGES = 131072
REGIONS = 256
N_ROW = 4
N_COL = 8


def with_ends(values, key, low, high):
    shape = values.shape
    index_at = [jax.random.randint(jax.random.fold_in(key, axis), (), 0, shape[axis]) for axis in range(len(shape))]
    values = values.at[tuple(index_at)].set(low)
    longest = shape.index(max(shape))
    index_at[longest] = (index_at[longest] + 1) % shape[longest]
    return values.at[tuple(index_at)].set(high)


def steps_of(stream_key, extent, cuts, least, top_value):
    factor_of = 1.0
    for position, shards_of in cuts:
        steps = jax.random.uniform(jax.random.fold_in(jax.random.fold_in(stream_key, 6), position), (shards_of,), jnp.float32, least / len(cuts), top_value / len(cuts))
        factor_of = factor_of * jnp.repeat(jnp.exp(steps), extent[position] // shards_of).reshape((-1,) + (1,) * (len(extent) - 1 - position))
    return factor_of


def bell_draw(stream_key, dims, deviation, reach, cuts=(), dtype=jnp.bfloat16):
    level = steps_of(stream_key, dims, cuts, -0.22, 0.18) if cuts else 1.0
    drawn = jax.random.normal(stream_key, dims, jnp.float32) * deviation * level
    return jnp.minimum(jnp.maximum(drawn, -reach), reach).astype(dtype)


def setup_inputs(seed: int = 0) -> dict:
    splits = jax.random.split(jax.random.key(seed), 17)
    node_latent = bell_draw(splits[0], (NODES, LATENT), 1.0, 6.0, ((0, 32),))
    edge_latent = bell_draw(splits[1], (EDGES, LATENT), 1.0, 6.0, ((0, 32),))
    senders = with_ends(jax.random.randint(splits[2], (EDGES,), 0, EXTENDED), jax.random.fold_in(splits[2], 1), 0, EXTENDED - 1).astype(jnp.int32)
    receivers = with_ends(jax.random.randint(splits[3], (EDGES,), 0, NODES_DEV), jax.random.fold_in(splits[3], 1), 0, NODES_DEV - 1).astype(jnp.int32)
    send_index = with_ends(jax.random.randint(splits[4], (PARTS_SIZE, 4, BOUNDARY), 0, NODES_DEV), jax.random.fold_in(splits[4], 1), 0, NODES_DEV - 1).astype(jnp.int32)
    context_table = bell_draw(splits[5], (REGIONS, LATENT), 1.0, 6.0, ((0, 32),))
    region = with_ends(jax.random.randint(splits[6], (NODES,), 0, REGIONS), jax.random.fold_in(splits[6], 1), 0, REGIONS - 1).astype(jnp.int32)
    edge_w1 = bell_draw(splits[7], (LAYERS, 3 * LATENT, LATENT), (3 * LATENT) ** -0.5, 0.3125)
    edge_w2 = bell_draw(splits[8], (LAYERS, LATENT, LATENT), LATENT ** -0.5, 0.5)
    edge_bias = bell_draw(splits[9], (LAYERS, 3, LATENT), 0.5, 3.0, (), jnp.float32)
    edge_gain = jnp.clip(1.0 + 0.15 * jax.random.normal(splits[10], (LAYERS, LATENT), jnp.float32), 0.25, 1.75)
    node_w1 = bell_draw(splits[11], (LAYERS, 3 * LATENT, LATENT), (3 * LATENT) ** -0.5, 0.3125)
    node_wg = bell_draw(splits[12], (LAYERS, LATENT, LATENT), LATENT ** -0.5, 0.5)
    node_w2 = bell_draw(splits[13], (LAYERS, LATENT, LATENT), LATENT ** -0.5, 0.5)
    node_bias = bell_draw(splits[14], (LAYERS, 3, LATENT), 0.5, 3.0, (), jnp.float32)
    node_gain = jnp.clip(1.0 + 0.15 * jax.random.normal(splits[15], (LAYERS, LATENT), jnp.float32), 0.25, 1.75)
    return dict(node_latent=node_latent, edge_latent=edge_latent, senders=senders, receivers=receivers, send_index=send_index, context_table=context_table, region=region, edge_w1=edge_w1, edge_w2=edge_w2, edge_bias=edge_bias, edge_gain=edge_gain, node_w1=node_w1, node_wg=node_wg, node_w2=node_w2, node_bias=node_bias, node_gain=node_gain)


EPS = 1e-05

def norm_tail(pre, w_out, b_out, gain, shift):
    hidden = jax.nn.relu(pre).astype(jnp.bfloat16)
    y_val = jnp.dot(hidden, w_out, preferred_element_type=jnp.float32) + b_out
    centred = y_val - lax.optimization_barrier(jnp.mean(y_val, axis=-1, keepdims=True))
    spread = lax.optimization_barrier(jnp.mean(centred * centred, axis=-1, keepdims=True))
    return centred * lax.rsqrt(spread + EPS) * gain + shift

def edge_step(extended, edges, senders, receivers, w_in, w_out, bias, gain):
    feats = jnp.concatenate([jnp.take(extended, senders, axis=0), jnp.take(extended, receivers, axis=0), edges], axis=1)
    pre = jnp.dot(feats, w_in, preferred_element_type=jnp.float32) + bias[0]
    return (edges.astype(jnp.float32) + norm_tail(pre, w_out, bias[1], gain, bias[2])).astype(jnp.bfloat16)

def node_step(nodes, new_edges, receivers, context_rows, w_in, w_out, bias, gain, shift_in):
    summed = jax.ops.segment_sum(new_edges.astype(jnp.float32), receivers, num_segments=nodes.shape[0]).astype(jnp.bfloat16)
    feats = jnp.concatenate([nodes, summed, context_rows], axis=1)
    pre = jnp.dot(feats, w_in, preferred_element_type=jnp.float32) + shift_in
    return (nodes.astype(jnp.float32) + norm_tail(pre, w_out, bias[1], gain, bias[2])).astype(jnp.bfloat16)

def pick_rows(nodes, index):
    width = nodes.shape[1]
    return jnp.take(nodes, index.reshape(-1), axis=0).reshape(4, index.shape[1], width)

def with_halo(nodes, send_index):
    sent = jax.vmap(jax.vmap(pick_rows))(nodes, send_index)
    zero_row = jnp.zeros_like(sent[:1, :, 0])
    from_above = jnp.concatenate([zero_row, sent[:-1, :, 0]], axis=0)
    from_below = jnp.concatenate([sent[1:, :, 1], zero_row], axis=0)
    zero_col = jnp.zeros_like(sent[:, :1, 2])
    from_left = jnp.concatenate([zero_col, sent[:, :-1, 2]], axis=1)
    from_right = jnp.concatenate([sent[:, 1:, 3], zero_col], axis=1)
    return jnp.concatenate([nodes, from_above, from_below, from_left, from_right], axis=2)

def reference(node_latent, edge_latent, senders, receivers, send_index, context_table, region, edge_w1, edge_w2, edge_bias, edge_gain, node_w1, node_wg, node_w2, node_bias, node_gain):
    width = node_latent.shape[1]
    pooled = lax.optimization_barrier(jnp.sum(node_latent.astype(jnp.float32), axis=0)) / math.sqrt(NODES)
    nodes = node_latent.reshape(N_ROW, N_COL, NODES_DEV, width)
    edges = edge_latent.reshape(PARTS_SIZE, EDGES_DEV, width)
    sender_rows = senders.reshape(PARTS_SIZE, EDGES_DEV)
    receiver_rows = receivers.reshape(PARTS_SIZE, EDGES_DEV)
    index = send_index.reshape(N_ROW, N_COL, 4, BOUNDARY)
    context_rows = jnp.take(context_table, region, axis=0).reshape(PARTS_SIZE, NODES_DEV, width)
    for layer in range(LAYERS):
        extended = with_halo(nodes, index).reshape(PARTS_SIZE, EXTENDED, width)
        flat = nodes.reshape(PARTS_SIZE, NODES_DEV, width)
        shift_in = node_bias[layer, 0] + jnp.dot(pooled, node_wg[layer].astype(jnp.float32), precision=lax.Precision.HIGHEST)

        def one_part(items, layer=layer, shift_in=shift_in):
            ext_p, edges_p, send_p, recv_p, nodes_p, ctx_p = items
            new_edges = edge_step(ext_p, edges_p, send_p, recv_p, edge_w1[layer], edge_w2[layer], edge_bias[layer], edge_gain[layer])
            new_nodes = node_step(nodes_p, new_edges, recv_p, ctx_p, node_w1[layer], node_w2[layer], node_bias[layer], node_gain[layer], shift_in)
            return (new_edges, new_nodes)
        edges, flat = lax.map(one_part, (extended, edges, sender_rows, receiver_rows, flat, context_rows))
        nodes = flat.reshape(N_ROW, N_COL, NODES_DEV, width)
    return (nodes.reshape(NODES, width), edges.reshape(EDGES, width))
```

```python
import functools
import math

import jax
import jax.numpy as jnp
from jax import lax
from jax.experimental import pallas as pl
from jax.experimental.pallas import tpu as pltpu
from jax.sharding import PartitionSpec as P

LAYERS = 2
EPS = 1e-05
LANES = 128
BLOCK = 512
F32 = jnp.float32
BF16 = jnp.bfloat16
MESH = pl.DeviceIdType.MESH


def mm(a, b):
    return jnp.dot(a, b, preferred_element_type=F32)


def iota(axis):
    return lax.broadcasted_iota(jnp.int32, (LANES, LANES), axis)


def as_column(row):
    return jnp.transpose(jnp.broadcast_to(row, (LANES, LANES)))


def hot(mask):
    return jnp.where(mask, 1.0, 0.0).astype(BF16)


def pick_rows(column, count):
    lanes = iota(1)
    parts = [hot(column == lanes + start) for start in range(0, count, LANES)]
    return jnp.concatenate(parts, axis=1)


def norm(y_val, gain, shift):
    centred = y_val - jnp.mean(y_val, axis=-1, keepdims=True)
    spread = jnp.mean(centred * centred, axis=-1, keepdims=True)
    return centred * lax.rsqrt(spread + EPS) * gain + shift


def kernel(
    n_row,
    n_col,
    node_ref,
    edge_ref,
    send_ref,
    recv_ref,
    index_ref,
    ctx_ref,
    region_ref,
    ew1,
    ew2,
    eb,
    eg,
    nw1,
    nwg,
    nw2,
    nb,
    ng,
    node_out,
    edge_out,
    hot_send,
    hot_recv,
    hot_sum,
    side_send,
    side_recv,
    hot_index,
    picked,
    halo,
    table,
    from_ext,
    from_own,
    sums,
    ctx_part,
    halo_send_sem,
    halo_recv_sem,
    row_send_sem,
    row_recv_sem,
    col_send_sem,
    col_recv_sem,
):
    my_row, my_col = lax.axis_index("row"), lax.axis_index("col")
    nodes, width = node_ref.shape
    edges = edge_ref.shape[0]
    count = index_ref.shape[1]
    ext = nodes + 4 * count
    half_ext, half_own = ext // 2, nodes // 2
    ctx_rows = ctx_ref.shape[0]
    per_block = BLOCK // LANES

    barrier = pltpu.get_barrier_semaphore()
    for step in range(1, n_row):
        pl.semaphore_signal(
            barrier, inc=1, device_id=(lax.rem(my_row + step, n_row), my_col), device_id_type=MESH
        )
    for step in range(1, n_col):
        pl.semaphore_signal(
            barrier, inc=1, device_id=(my_row, lax.rem(my_col + step, n_col)), device_id_type=MESH
        )

    for side in range(4):
        rows = slice(side * count, (side + 1) * count)
        hot_index[rows, :] = pick_rows(as_column(index_ref[side : side + 1, :]), nodes)
    picked[0] = mm(hot_index[...], node_ref[...]).astype(BF16)
    part = jnp.sum(node_ref[...].astype(F32).reshape(nodes // 8, 8, width), axis=0)
    table[my_col, my_row] = jnp.concatenate([ctx_ref[...].astype(F32), part], axis=0)

    pl.semaphore_wait(barrier, n_row + n_col - 2)

    moves = (
        (my_row + 1, my_col, my_row < n_row - 1, my_row > 0),
        (my_row - 1, my_col, my_row > 0, my_row < n_row - 1),
        (my_row, my_col + 1, my_col < n_col - 1, my_col > 0),
        (my_row, my_col - 1, my_col > 0, my_col < n_col - 1),
    )

    def halo_copy(layer, side):
        to_row, to_col = moves[side][:2]
        rows = pl.ds(side * count, count)
        return pltpu.make_async_remote_copy(
            src_ref=picked.at[layer, rows],
            dst_ref=halo.at[layer, rows],
            send_sem=halo_send_sem.at[layer, side],
            recv_sem=halo_recv_sem.at[layer, side],
            device_id=(to_row, to_col),
            device_id_type=MESH,
        )

    def halo_start(layer):
        for side in range(4):

            @pl.when(moves[side][2])
            def _(side=side):
                halo_copy(layer, side).start()

    def halo_wait(layer):
        for side in range(4):

            @pl.when(moves[side][3])
            def _(side=side):
                halo_copy(layer, side).wait_recv()

            @pl.when(jnp.logical_not(moves[side][3]))
            def _(side=side):
                halo[layer, side * count : (side + 1) * count] = jnp.zeros((count, width), BF16)

    def row_copy(step, owner):
        return pltpu.make_async_remote_copy(
            src_ref=table.at[my_col, owner],
            dst_ref=table.at[my_col, owner],
            send_sem=row_send_sem.at[step - 1],
            recv_sem=row_recv_sem.at[step - 1],
            device_id=(lax.rem(my_row + step, n_row), my_col),
            device_id_type=MESH,
        )

    def col_copy(step, owner):
        return pltpu.make_async_remote_copy(
            src_ref=table.at[owner],
            dst_ref=table.at[owner],
            send_sem=col_send_sem.at[step - 1],
            recv_sem=col_recv_sem.at[step - 1],
            device_id=(my_row, lax.rem(my_col + step, n_col)),
            device_id_type=MESH,
        )

    halo_start(0)
    for step in range(1, n_row):
        row_copy(step, my_row).start()

    def prepare(block, carry):
        for sub in range(per_block):
            line = block * per_block + sub
            send_row = send_ref[pl.ds(line, 1), :]
            recv_row = recv_ref[pl.ds(line, 1), :]
            rows = pl.ds(pl.multiple_of(line * LANES, LANES), LANES)
            send = as_column(send_row)
            recv = as_column(recv_row)
            send_high = (send >= half_ext).astype(jnp.int32)
            recv_high = (recv >= half_own).astype(jnp.int32)
            side_send[rows, :] = send_high
            side_recv[rows, :] = recv_high
            hot_send[rows, :] = pick_rows(send - send_high * half_ext, half_ext)
            hot_recv[rows, :] = pick_rows(recv - recv_high * half_own, half_own)
            recv_low = recv_row - (recv_row >= half_own).astype(jnp.int32) * half_own
            for start in range(0, half_own, LANES):
                hot_sum[block, start : start + LANES, sub * LANES : (sub + 1) * LANES] = hot(
                    iota(0) + start == recv_low
                )
        return carry

    lax.fori_loop(0, edges // BLOCK, prepare, 0)

    for step in range(1, n_row):
        row_copy(step, lax.rem(my_row + n_row - step, n_row)).wait_recv()
    for step in range(1, n_col):
        col_copy(step, my_col).start()

    def fill_own(layer, now):
        w_pair = jnp.concatenate([ew1[layer, :width], ew1[layer, width : 2 * width]], axis=1)
        both = mm(now[...], w_pair).astype(BF16)
        from_ext[:, :width] = both[:half_ext, :width]
        from_ext[: nodes - half_ext, width:] = both[half_ext:, :width]
        from_own[:, :width] = both[:half_own, width:]
        from_own[:, width:] = both[half_own:, width:]

    def edge_phase(layer, source):
        from_ext[nodes - half_ext :, width:] = mm(halo[layer], ew1[layer, :width]).astype(BF16)
        sums[...] = jnp.zeros_like(sums)

        def body(block, carry):
            rows = pl.ds(pl.multiple_of(block * BLOCK, BLOCK), BLOCK)
            old = source[rows, :]
            by_send = mm(hot_send[rows, :], from_ext[...])
            by_recv = mm(hot_recv[rows, :], from_own[...])
            high = side_recv[rows, :] > 0
            pre = mm(old, ew1[layer, 2 * width :]) + eb[layer, 0:1]
            pre += jnp.where(side_send[rows, :] > 0, by_send[:, width:], by_send[:, :width])
            pre += jnp.where(high, by_recv[:, width:], by_recv[:, :width])
            hidden = jnp.maximum(pre, 0.0).astype(BF16)
            y_val = mm(hidden, ew2[layer]) + eb[layer, 1:2]
            new = old.astype(F32) + norm(y_val, eg[layer : layer + 1], eb[layer, 2:3])
            edge_out[rows, :] = new.astype(BF16)
            low_part = jnp.where(high, 0.0, new).astype(BF16)
            high_part = jnp.where(high, new, 0.0).astype(BF16)
            sums[...] += mm(hot_sum[block], jnp.concatenate([low_part, high_part], axis=1))
            return carry

        lax.fori_loop(0, edges // BLOCK, body, 0)

    def node_phase(layer, now, shift_in):
        summed = jnp.concatenate([sums[:, :width], sums[:, width:]], axis=0).astype(BF16)
        feats = jnp.concatenate([now[...], summed], axis=1)
        pre = mm(feats, nw1[layer, : 2 * width]) + shift_in
        pre += ctx_part[:, layer * width : (layer + 1) * width]
        hidden = jnp.maximum(pre, 0.0).astype(BF16)
        y_val = mm(hidden, nw2[layer]) + nb[layer, 1:2]
        new = now[...].astype(F32) + norm(y_val, ng[layer : layer + 1], nb[layer, 2:3])
        node_out[...] = new.astype(BF16)

    fill_own(0, node_ref)
    halo_wait(0)
    edge_phase(0, edge_ref)

    for step in range(1, n_col):
        col_copy(step, lax.rem(my_col + n_col - step, n_col)).wait_recv()
    pooled_sum = jnp.zeros((8, width), F32)
    shared = []
    for row in range(n_row):
        for col in range(n_col):
            shared.append(table[col, row, :ctx_rows])
            pooled_sum += table[col, row, ctx_rows:]
    pooled = jnp.sum(pooled_sum, axis=0, keepdims=True) / math.sqrt(nodes * n_row * n_col)
    regions = n_row * n_col * ctx_rows
    w_pair = jnp.concatenate([nw1[l, 2 * width :] for l in range(LAYERS)], axis=1)
    projected = mm(jnp.concatenate(shared, axis=0).astype(BF16), w_pair).astype(BF16)
    for line in range(nodes // LANES):
        picker = pick_rows(as_column(region_ref[line : line + 1, :]), regions)
        ctx_part[line * LANES : (line + 1) * LANES, :] = mm(picker, projected)
    shifts = [
        nb[l, 0:1]
        + jnp.dot(
            pooled, nwg[l].astype(F32), precision=lax.Precision.HIGHEST, preferred_element_type=F32
        )
        for l in range(LAYERS)
    ]
    node_phase(0, node_ref, shifts[0])

    picked[1] = mm(hot_index[...], node_out[...]).astype(BF16)
    halo_start(1)
    fill_own(1, node_out)
    halo_wait(1)
    edge_phase(1, edge_out)
    node_phase(1, node_out, shifts[1])

    for layer in range(LAYERS):
        for side in range(4):

            @pl.when(moves[side][2])
            def _(layer=layer, side=side):
                halo_copy(layer, side).wait_send()

    for step in range(1, n_row):
        row_copy(step, my_row).wait_send()
    for step in range(1, n_col):
        col_copy(step, my_col).wait_send()


def local(n_row, n_col, *args):
    node, edge, send, recv, index, ctx, region = args[:7]
    nodes, width = node.shape
    edges = edge.shape[0]
    count = index.shape[2]
    half_ext, half_own = (nodes + 4 * count) // 2, nodes // 2
    vmem = pl.BlockSpec(memory_space=pltpu.VMEM)
    dma = pltpu.SemaphoreType.DMA
    operands = (
        node,
        edge,
        send.reshape(edges // LANES, LANES),
        recv.reshape(edges // LANES, LANES),
        index.reshape(4, count),
        ctx,
        region.reshape(nodes // LANES, LANES),
    ) + args[7:]
    return pl.pallas_call(
        functools.partial(kernel, n_row, n_col),
        out_shape=(
            jax.ShapeDtypeStruct(node.shape, BF16),
            jax.ShapeDtypeStruct(edge.shape, BF16),
        ),
        in_specs=[vmem] * len(operands),
        out_specs=(vmem, vmem),
        scratch_shapes=[
            pltpu.VMEM((edges, half_ext), BF16),
            pltpu.VMEM((edges, half_own), BF16),
            pltpu.VMEM((edges // BLOCK, half_own, BLOCK), BF16),
            pltpu.VMEM((edges, width), jnp.int32),
            pltpu.VMEM((edges, width), jnp.int32),
            pltpu.VMEM((4 * count, nodes), BF16),
            pltpu.VMEM((LAYERS, 4 * count, width), BF16),
            pltpu.VMEM((LAYERS, 4 * count, width), BF16),
            pltpu.VMEM((n_col, n_row, ctx.shape[0] + 8, width), F32),
            pltpu.VMEM((half_ext, 2 * width), BF16),
            pltpu.VMEM((half_own, 2 * width), BF16),
            pltpu.VMEM((half_own, 2 * width), F32),
            pltpu.VMEM((nodes, LAYERS * width), F32),
            dma((LAYERS, 4)),
            dma((LAYERS, 4)),
            dma((n_row - 1,)),
            dma((n_row - 1,)),
            dma((n_col - 1,)),
            dma((n_col - 1,)),
        ],
        compiler_params=pltpu.CompilerParams(
            collective_id=0, has_side_effects=True, vmem_limit_bytes=56 * 1024 * 1024
        ),
        name="mesh_steps",
    )(*operands)


def solution(mesh):
    both = ("row", "col")
    split = (P(both, None), P(both, None), P(both), P(both), P(both, None, None), P(both, None), P(both))
    return jax.shard_map(
        functools.partial(local, mesh.shape["row"], mesh.shape["col"]),
        mesh=mesh,
        in_specs=split + (P(),) * 9,
        out_specs=(P(both, None), P(both, None)),
        check_vma=False,
    )
```

```python
import functools
import math

import jax
import jax.numpy as jnp
from jax import lax
from jax.experimental import pallas as pl
from jax.experimental.pallas import tpu as pltpu
from jax.sharding import PartitionSpec as P

LAYERS = 2
EPS = 1e-05
LANES = 128
BLOCK = 512
F32 = jnp.float32
BF16 = jnp.bfloat16
MESH = pl.DeviceIdType.MESH


def mm(a, b):
    return jnp.dot(a, b, preferred_element_type=F32)


def iota(axis):
    return lax.broadcasted_iota(jnp.int32, (LANES, LANES), axis)


def as_column(row):
    return jnp.transpose(jnp.broadcast_to(row, (LANES, LANES)))


def hot(mask):
    return jnp.where(mask, 1.0, 0.0).astype(BF16)


def pick_parts(index, axis, count):
    base = hot((index & (LANES - 1)) == iota(axis))
    group = (index >> 7).astype(F32).astype(BF16)
    zero = jnp.zeros_like(base)
    return [
        jnp.where(group == jnp.asarray(part, BF16), base, zero) for part in range(count // LANES)
    ]


def pick_rows(column, count):
    return jnp.concatenate(pick_parts(column, 1, count), axis=1)


def centre(values):
    values = values.astype(F32)
    return values - jnp.mean(values, axis=-1, keepdims=True)


def norm(centred, gain, shift):
    spread = jnp.mean(centred * centred, axis=-1, keepdims=True)
    return centred * lax.rsqrt(spread + EPS) * gain + shift


def kernel(
    n_row,
    n_col,
    node_ref,
    edge_ref,
    send_ref,
    recv_ref,
    index_ref,
    ctx_ref,
    region_ref,
    ew1,
    ew2,
    eb,
    eg,
    nw1,
    nwg,
    nw2,
    nb,
    ng,
    node_out,
    edge_out,
    operand,
    hot_sum,
    side_send,
    side_recv,
    hot_index,
    picked,
    halo,
    table,
    weights,
    sums,
    ctx_part,
    even_part,
    odd_part,
    edge_sem,
    halo_send_sem,
    halo_recv_sem,
    row_send_sem,
    row_recv_sem,
    col_send_sem,
    col_recv_sem,
):
    my_row, my_col = lax.axis_index("row"), lax.axis_index("col")
    nodes, width = node_ref.shape
    edges = edge_ref.shape[0]
    count = index_ref.shape[1]
    ext = nodes + 4 * count
    half_ext, half_own = ext // 2, nodes // 2
    ctx_rows = ctx_ref.shape[0]
    at_recv, at_edge = half_ext, half_ext + nodes
    edge_in = pltpu.make_async_copy(
        edge_ref, operand.at[:, at_edge : at_edge + width], edge_sem
    )
    edge_in.start()
    per_block = BLOCK // LANES

    barrier = pltpu.get_barrier_semaphore()
    for step in range(1, n_row):
        pl.semaphore_signal(
            barrier, inc=1, device_id=(lax.rem(my_row + step, n_row), my_col), device_id_type=MESH
        )
    for step in range(1, n_col):
        pl.semaphore_signal(
            barrier, inc=1, device_id=(my_row, lax.rem(my_col + step, n_col)), device_id_type=MESH
        )

    for side in range(4):
        rows = slice(side * count, (side + 1) * count)
        hot_index[rows, :] = pick_rows(as_column(index_ref[side : side + 1, :]), nodes)
    picked[0] = mm(hot_index[...], node_ref[...]).astype(BF16)
    part = jnp.sum(node_ref[...].astype(F32).reshape(nodes // 8, 8, width), axis=0)
    table[my_col, my_row] = jnp.concatenate([ctx_ref[...].astype(F32), part], axis=0)

    pl.semaphore_wait(barrier, n_row + n_col - 2)

    moves = (
        (my_row + 1, my_col, my_row < n_row - 1, my_row > 0),
        (my_row - 1, my_col, my_row > 0, my_row < n_row - 1),
        (my_row, my_col + 1, my_col < n_col - 1, my_col > 0),
        (my_row, my_col - 1, my_col > 0, my_col < n_col - 1),
    )

    def halo_copy(layer, side):
        to_row, to_col = moves[side][:2]
        rows = pl.ds(side * count, count)
        return pltpu.make_async_remote_copy(
            src_ref=picked.at[layer, rows],
            dst_ref=halo.at[layer, rows],
            send_sem=halo_send_sem.at[layer, side],
            recv_sem=halo_recv_sem.at[layer, side],
            device_id=(to_row, to_col),
            device_id_type=MESH,
        )

    def halo_start(layer):
        for side in range(4):

            @pl.when(moves[side][2])
            def _(side=side):
                halo_copy(layer, side).start()

    def halo_wait(layer):
        for side in range(4):

            @pl.when(moves[side][3])
            def _(side=side):
                halo_copy(layer, side).wait_recv()

            @pl.when(jnp.logical_not(moves[side][3]))
            def _(side=side):
                halo[layer, side * count : (side + 1) * count] = jnp.zeros((count, width), BF16)

    def row_copy(step, owner):
        return pltpu.make_async_remote_copy(
            src_ref=table.at[my_col, owner],
            dst_ref=table.at[my_col, owner],
            send_sem=row_send_sem.at[step - 1],
            recv_sem=row_recv_sem.at[step - 1],
            device_id=(lax.rem(my_row + step, n_row), my_col),
            device_id_type=MESH,
        )

    def col_copy(step, owner):
        return pltpu.make_async_remote_copy(
            src_ref=table.at[owner],
            dst_ref=table.at[owner],
            send_sem=col_send_sem.at[step - 1],
            recv_sem=col_recv_sem.at[step - 1],
            device_id=(my_row, lax.rem(my_col + step, n_col)),
            device_id_type=MESH,
        )

    halo_start(0)
    for step in range(1, n_row):
        row_copy(step, my_row).start()

    def prepare(block, carry):
        for sub in range(per_block):
            line = block * per_block + sub
            send_row = send_ref[pl.ds(line, 1), :]
            recv_row = recv_ref[pl.ds(line, 1), :]
            rows = pl.ds(pl.multiple_of(line * LANES, LANES), LANES)
            both = as_column(send_row + (recv_row << 16))
            send, recv = both & 0xFFFF, both >> 16
            send_high = (send >= half_ext).astype(jnp.int32)
            side_send[rows, :] = send_high
            side_recv[rows, :] = (recv >= half_own).astype(jnp.int32)
            operand[rows, :at_recv] = pick_rows(send - send_high * half_ext, half_ext)
            operand[rows, at_recv:at_edge] = pick_rows(recv, nodes)
            recv_low = recv_row - (recv_row >= half_own).astype(jnp.int32) * half_own
            recv_low = jnp.broadcast_to(recv_low, (LANES, LANES))
            for part, value in enumerate(pick_parts(recv_low, 0, half_own)):
                hot_sum[
                    block, part * LANES : (part + 1) * LANES, sub * LANES : (sub + 1) * LANES
                ] = value
        return carry

    lax.fori_loop(0, edges // BLOCK, prepare, 0)

    for step in range(1, n_row):
        row_copy(step, lax.rem(my_row + n_row - step, n_row)).wait_recv()
    for step in range(1, n_col):
        col_copy(step, my_col).start()

    def fill_own(layer, now):
        w_pair = jnp.concatenate([ew1[layer, :width], ew1[layer, width : 2 * width]], axis=1)
        both = mm(now[...], w_pair).astype(BF16)
        weights[:half_ext, :width] = both[:half_ext, :width]
        weights[: nodes - half_ext, width:] = both[half_ext:, :width]
        for start in (0, width):
            weights[at_recv:at_edge, start : start + width] = both[:, width:]
            weights[at_edge:, start : start + width] = ew1[layer, 2 * width :]

    def edge_phase(layer):
        weights[nodes - half_ext : half_ext, width:] = mm(halo[layer], ew1[layer, :width]).astype(
            BF16
        )
        sums[...] = jnp.zeros_like(sums)
        odd_part[...] = jnp.zeros_like(odd_part)
        w_out = centre(ew2[layer]).astype(BF16)
        b_out = centre(eb[1, layer : layer + 1])

        def gather(block, target):
            rows = pl.ds(pl.multiple_of(block * BLOCK, BLOCK), BLOCK)
            pre = mm(operand[rows, :], weights[...])
            pre = jnp.where(side_send[rows, :] > 0, pre[:, width:], pre[:, :width])
            hidden = jnp.maximum(pre + eb[0, layer : layer + 1], 0.0).astype(BF16)
            centred = mm(hidden, w_out) + b_out
            new = operand[rows, at_edge:].astype(F32)
            new += norm(centred, eg[layer : layer + 1], eb[2, layer : layer + 1])
            if layer == LAYERS - 1:
                edge_out[rows, :] = new.astype(BF16)
            else:
                operand[rows, at_edge:] = new.astype(BF16)
            high = side_recv[rows, :] > 0
            target[:, :width] = jnp.where(high, 0.0, new).astype(BF16)
            target[:, width:] = jnp.where(high, new, 0.0).astype(BF16)

        def scatter(block, source):
            sums[...] += mm(hot_sum[block], source[...])

        def body(pair, carry):
            scatter(jnp.maximum(2 * pair - 1, 0), odd_part)
            gather(2 * pair, even_part)
            scatter(2 * pair, even_part)
            gather(2 * pair + 1, odd_part)
            return carry

        lax.fori_loop(0, edges // (2 * BLOCK), body, 0)
        scatter(edges // BLOCK - 1, odd_part)

    def node_phase(layer, now, shift_in):
        summed = jnp.concatenate([sums[:, :width], sums[:, width:]], axis=0).astype(BF16)
        feats = jnp.concatenate([now[...], summed], axis=1)
        pre = mm(feats, nw1[layer, : 2 * width]) + shift_in
        pre += ctx_part[:, layer * width : (layer + 1) * width]
        hidden = jnp.maximum(pre, 0.0).astype(BF16)
        centred = mm(hidden, centre(nw2[layer]).astype(BF16)) + centre(nb[1, layer : layer + 1])
        new = now[...].astype(F32)
        new += norm(centred, ng[layer : layer + 1], nb[2, layer : layer + 1])
        node_out[...] = new.astype(BF16)

    fill_own(0, node_ref)
    halo_wait(0)
    edge_in.wait()
    edge_phase(0)

    for step in range(1, n_col):
        col_copy(step, lax.rem(my_col + n_col - step, n_col)).wait_recv()
    pooled_sum = jnp.zeros((8, width), F32)
    shared = []
    for row in range(n_row):
        for col in range(n_col):
            shared.append(table[col, row, :ctx_rows])
            pooled_sum += table[col, row, ctx_rows:]
    pooled = jnp.sum(pooled_sum, axis=0, keepdims=True) / math.sqrt(nodes * n_row * n_col)
    regions = n_row * n_col * ctx_rows
    w_pair = jnp.concatenate([nw1[l, 2 * width :] for l in range(LAYERS)], axis=1)
    projected = mm(jnp.concatenate(shared, axis=0).astype(BF16), w_pair).astype(BF16)
    for line in range(nodes // LANES):
        picker = pick_rows(as_column(region_ref[line : line + 1, :]), regions)
        ctx_part[line * LANES : (line + 1) * LANES, :] = mm(picker, projected)
    shifts = [
        nb[0, l : l + 1]
        + jnp.dot(
            pooled, nwg[l].astype(F32), precision=lax.Precision.HIGHEST, preferred_element_type=F32
        )
        for l in range(LAYERS)
    ]
    node_phase(0, node_ref, shifts[0])

    picked[1] = mm(hot_index[...], node_out[...]).astype(BF16)
    halo_start(1)
    fill_own(1, node_out)
    halo_wait(1)
    edge_phase(1)
    node_phase(1, node_out, shifts[1])

    for layer in range(LAYERS):
        for side in range(4):

            @pl.when(moves[side][2])
            def _(layer=layer, side=side):
                halo_copy(layer, side).wait_send()

    for step in range(1, n_row):
        row_copy(step, my_row).wait_send()
    for step in range(1, n_col):
        col_copy(step, my_col).wait_send()


def local(n_row, n_col, *args):
    node, edge, send, recv, index, ctx, region = args[:7]
    nodes, width = node.shape
    edges = edge.shape[0]
    count = index.shape[2]
    half_ext, half_own = (nodes + 4 * count) // 2, nodes // 2
    deep = half_ext + nodes + width
    vmem = pl.BlockSpec(memory_space=pltpu.VMEM)
    dma = pltpu.SemaphoreType.DMA
    operands = (
        node,
        edge,
        send.reshape(edges // LANES, LANES),
        recv.reshape(edges // LANES, LANES),
        index.reshape(4, count),
        ctx,
        region.reshape(nodes // LANES, LANES),
    ) + args[7:]
    operands = tuple(
        jnp.transpose(x, (1, 0, 2)) if x.shape == (LAYERS, 3, width) else x for x in operands
    )
    return pl.pallas_call(
        functools.partial(kernel, n_row, n_col),
        out_shape=(
            jax.ShapeDtypeStruct(node.shape, BF16),
            jax.ShapeDtypeStruct(edge.shape, BF16),
        ),
        in_specs=[vmem, pl.BlockSpec(memory_space=pl.ANY)] + [vmem] * (len(operands) - 2),
        out_specs=(vmem, vmem),
        scratch_shapes=[
            pltpu.VMEM((edges, deep), BF16),
            pltpu.VMEM((edges // BLOCK, half_own, BLOCK), BF16),
            pltpu.VMEM((edges, width), jnp.int32),
            pltpu.VMEM((edges, width), jnp.int32),
            pltpu.VMEM((4 * count, nodes), BF16),
            pltpu.VMEM((LAYERS, 4 * count, width), BF16),
            pltpu.VMEM((LAYERS, 4 * count, width), BF16),
            pltpu.VMEM((n_col, n_row, ctx.shape[0] + 8, width), F32),
            pltpu.VMEM((deep, 2 * width), BF16),
            pltpu.VMEM((half_own, 2 * width), F32),
            pltpu.VMEM((nodes, LAYERS * width), F32),
            pltpu.VMEM((BLOCK, 2 * width), BF16),
            pltpu.VMEM((BLOCK, 2 * width), BF16),
            dma(()),
            dma((LAYERS, 4)),
            dma((LAYERS, 4)),
            dma((n_row - 1,)),
            dma((n_row - 1,)),
            dma((n_col - 1,)),
            dma((n_col - 1,)),
        ],
        compiler_params=pltpu.CompilerParams(
            collective_id=0, has_side_effects=True, vmem_limit_bytes=56 * 1024 * 1024
        ),
        name="mesh_steps",
    )(*operands)


def solution(mesh):
    both = ("row", "col")
    split = (P(both, None), P(both, None), P(both), P(both), P(both, None, None), P(both, None), P(both))
    return jax.shard_map(
        functools.partial(local, mesh.shape["row"], mesh.shape["col"]),
        mesh=mesh,
        in_specs=split + (P(),) * 9,
        out_specs=(P(both, None), P(both, None)),
        check_vma=False,
    )
```

```python
import functools
import math

import jax
import jax.numpy as jnp
from jax import lax
from jax.experimental import pallas as pl
from jax.experimental.pallas import tpu as pltpu
from jax.sharding import PartitionSpec as P

LAYERS = 2
EPS = 1e-05
LANES = 128
BLOCK = 512
F32 = jnp.float32
BF16 = jnp.bfloat16
MESH = pl.DeviceIdType.MESH


def mm(a, b):
    return jnp.dot(a, b, preferred_element_type=F32)


def iota(axis):
    return lax.broadcasted_iota(jnp.int32, (LANES, LANES), axis)


def as_column(row):
    return jnp.transpose(jnp.broadcast_to(row, (LANES, LANES)))


def hot(mask):
    return jnp.where(mask, 1.0, 0.0).astype(BF16)


def pick_parts(index, axis, count):
    base = hot((index & (LANES - 1)) == iota(axis))
    group = (index >> 7).astype(F32).astype(BF16)
    zero = jnp.zeros_like(base)
    return [
        jnp.where(group == jnp.asarray(part, BF16), base, zero) for part in range(count // LANES)
    ]


def pick_rows(column, count):
    return jnp.concatenate(pick_parts(column, 1, count), axis=1)


def centre(values):
    values = values.astype(F32)
    return values - jnp.mean(values, axis=-1, keepdims=True)


def twice(weight):
    zero = jnp.zeros_like(weight)
    top = jnp.concatenate([weight, zero], axis=1)
    return jnp.concatenate([top, jnp.concatenate([zero, weight], axis=1)], axis=0)


def norm(centred, gain, shift):
    spread = jnp.mean(centred * centred, axis=-1, keepdims=True)
    return centred * lax.rsqrt(spread + EPS) * gain + shift


def kernel(
    n_row,
    n_col,
    node_ref,
    edge_ref,
    send_ref,
    recv_ref,
    index_ref,
    ctx_ref,
    region_ref,
    ew1,
    ew2,
    eb,
    eg,
    nw1,
    nwg,
    nw2,
    nb,
    ng,
    node_out,
    edge_out,
    hot_send,
    hot_recv,
    hot_sum,
    side_send,
    side_recv,
    hot_index,
    picked,
    halo,
    table,
    from_ext,
    from_own,
    sums,
    ctx_part,
    parts,
    edge_sem,
    halo_send_sem,
    halo_recv_sem,
    row_send_sem,
    row_recv_sem,
    col_send_sem,
    col_recv_sem,
):
    my_row, my_col = lax.axis_index("row"), lax.axis_index("col")
    nodes, width = node_ref.shape
    edges = edge_ref.shape[0]
    count = index_ref.shape[1]
    ext = nodes + 4 * count
    half_ext, half_own = ext // 2, nodes // 2
    ctx_rows = ctx_ref.shape[0]
    edge_in = pltpu.make_async_copy(edge_ref, edge_out, edge_sem)
    edge_in.start()
    per_block = 2 * BLOCK // LANES

    barrier = pltpu.get_barrier_semaphore()
    for step in range(1, n_row):
        pl.semaphore_signal(
            barrier, inc=1, device_id=(lax.rem(my_row + step, n_row), my_col), device_id_type=MESH
        )
    for step in range(1, n_col):
        pl.semaphore_signal(
            barrier, inc=1, device_id=(my_row, lax.rem(my_col + step, n_col)), device_id_type=MESH
        )

    for side in range(4):
        rows = slice(side * count, (side + 1) * count)
        hot_index[rows, :] = pick_rows(as_column(index_ref[side : side + 1, :]), nodes)
    picked[0] = mm(hot_index[...], node_ref[...]).astype(BF16)
    part = jnp.sum(node_ref[...].astype(F32).reshape(nodes // 8, 8, width), axis=0)
    table[my_col, my_row] = jnp.concatenate([ctx_ref[...].astype(F32), part], axis=0)

    pl.semaphore_wait(barrier, n_row + n_col - 2)

    moves = (
        (my_row + 1, my_col, my_row < n_row - 1, my_row > 0),
        (my_row - 1, my_col, my_row > 0, my_row < n_row - 1),
        (my_row, my_col + 1, my_col < n_col - 1, my_col > 0),
        (my_row, my_col - 1, my_col > 0, my_col < n_col - 1),
    )

    def halo_copy(layer, side):
        to_row, to_col = moves[side][:2]
        rows = pl.ds(side * count, count)
        return pltpu.make_async_remote_copy(
            src_ref=picked.at[layer, rows],
            dst_ref=halo.at[layer, rows],
            send_sem=halo_send_sem.at[layer, side],
            recv_sem=halo_recv_sem.at[layer, side],
            device_id=(to_row, to_col),
            device_id_type=MESH,
        )

    def halo_start(layer):
        for side in range(4):

            @pl.when(moves[side][2])
            def _(side=side):
                halo_copy(layer, side).start()

    def halo_wait(layer):
        for side in range(4):

            @pl.when(moves[side][3])
            def _(side=side):
                halo_copy(layer, side).wait_recv()

            @pl.when(jnp.logical_not(moves[side][3]))
            def _(side=side):
                halo[layer, side * count : (side + 1) * count] = jnp.zeros((count, width), BF16)

    def row_copy(step, owner):
        return pltpu.make_async_remote_copy(
            src_ref=table.at[my_col, owner],
            dst_ref=table.at[my_col, owner],
            send_sem=row_send_sem.at[step - 1],
            recv_sem=row_recv_sem.at[step - 1],
            device_id=(lax.rem(my_row + step, n_row), my_col),
            device_id_type=MESH,
        )

    def col_copy(step, owner):
        return pltpu.make_async_remote_copy(
            src_ref=table.at[owner],
            dst_ref=table.at[owner],
            send_sem=col_send_sem.at[step - 1],
            recv_sem=col_recv_sem.at[step - 1],
            device_id=(my_row, lax.rem(my_col + step, n_col)),
            device_id_type=MESH,
        )

    halo_start(0)
    for step in range(1, n_row):
        row_copy(step, my_row).start()

    def prepare(block, carry):
        for sub in range(per_block):
            line = block * per_block + sub
            send_row = send_ref[pl.ds(line, 1), :]
            recv_row = recv_ref[pl.ds(line, 1), :]
            rows = pl.ds(pl.multiple_of(line * LANES, LANES), LANES)
            both = as_column(send_row + (recv_row << 16))
            send, recv = both & 0xFFFF, both >> 16
            send_high = (send >= half_ext).astype(jnp.int32)
            side_send[rows, :] = send_high
            recv_high = (recv >= half_own).astype(jnp.int32)
            side_recv[rows, :] = recv_high
            hot_send[rows, :] = pick_rows(send - send_high * half_ext, half_ext)
            hot_recv[rows, :] = pick_rows(recv - recv_high * half_own, half_own)
            recv_low = recv_row - (recv_row >= half_own).astype(jnp.int32) * half_own
            recv_low = jnp.broadcast_to(recv_low, (LANES, LANES))
            for part, value in enumerate(pick_parts(recv_low, 0, half_own)):
                hot_sum[
                    block, part * LANES : (part + 1) * LANES, sub * LANES : (sub + 1) * LANES
                ] = value
        return carry

    lax.fori_loop(0, edges // (2 * BLOCK), prepare, 0)

    for step in range(1, n_row):
        row_copy(step, lax.rem(my_row + n_row - step, n_row)).wait_recv()
    for step in range(1, n_col):
        col_copy(step, my_col).start()

    def fill_own(layer, now):
        w_pair = jnp.concatenate([ew1[layer, :width], ew1[layer, width : 2 * width]], axis=1)
        both = mm(now[...], w_pair).astype(BF16)
        from_ext[:, :width] = both[:half_ext, :width]
        from_ext[: nodes - half_ext, width:] = both[half_ext:, :width]
        from_own[:, :width] = both[:half_own, width:]
        from_own[:, width:] = both[half_own:, width:]

    def edge_phase(layer):
        from_ext[nodes - half_ext :, width:] = mm(halo[layer], ew1[layer, :width]).astype(BF16)
        sums[...] = jnp.zeros_like(sums)
        parts[...] = jnp.zeros_like(parts)
        w_edge = twice(ew1[layer, 2 * width :])
        w_out = twice(centre(ew2[layer]).astype(BF16))
        b_in = eb[0, layer : layer + 1]
        b_out = centre(eb[1, layer : layer + 1])

        def scatter(pair):
            sums[...] += mm(hot_sum[pair], parts[...])

        def body(pair, carry):
            blocks = [
                pl.ds(pl.multiple_of((2 * pair + half) * BLOCK, BLOCK), BLOCK) for half in range(2)
            ]
            old = [edge_out[rows, :] for rows in blocks]
            by_edge = mm(jnp.concatenate(old, axis=1), w_edge)
            by_send = [mm(hot_send[rows, :], from_ext[...]) for rows in blocks]
            by_recv = [mm(hot_recv[rows, :], from_own[...]) for rows in blocks]
            scatter(jnp.maximum(pair - 1, 0))
            hidden = []
            for half, rows in enumerate(blocks):
                pre = by_edge[:, half * width : (half + 1) * width] + b_in
                pre += jnp.where(
                    side_send[rows, :] > 0, by_send[half][:, width:], by_send[half][:, :width]
                )
                pre += jnp.where(
                    side_recv[rows, :] > 0, by_recv[half][:, width:], by_recv[half][:, :width]
                )
                hidden.append(jnp.maximum(pre, 0.0).astype(BF16))
            y_val = mm(jnp.concatenate(hidden, axis=1), w_out)
            for half, rows in enumerate(blocks):
                centred = y_val[:, half * width : (half + 1) * width] + b_out
                new = old[half].astype(F32)
                new += norm(centred, eg[layer : layer + 1], eb[2, layer : layer + 1])
                edge_out[rows, :] = new.astype(BF16)
                high = side_recv[rows, :] > 0
                place = slice(half * BLOCK, (half + 1) * BLOCK)
                parts[place, :width] = jnp.where(high, 0.0, new).astype(BF16)
                parts[place, width:] = jnp.where(high, new, 0.0).astype(BF16)
            return carry

        pairs = edges // (2 * BLOCK)
        lax.fori_loop(0, pairs, body, 0)
        scatter(pairs - 1)

    def node_phase(layer, now, shift_in):
        summed = jnp.concatenate([sums[:, :width], sums[:, width:]], axis=0).astype(BF16)
        feats = jnp.concatenate([now[...], summed], axis=1)
        pre = mm(feats, nw1[layer, : 2 * width]) + shift_in
        pre += ctx_part[:, layer * width : (layer + 1) * width]
        hidden = jnp.maximum(pre, 0.0).astype(BF16)
        centred = mm(hidden, centre(nw2[layer]).astype(BF16)) + centre(nb[1, layer : layer + 1])
        new = now[...].astype(F32)
        new += norm(centred, ng[layer : layer + 1], nb[2, layer : layer + 1])
        node_out[...] = new.astype(BF16)

    fill_own(0, node_ref)
    halo_wait(0)
    edge_in.wait()
    edge_phase(0)

    for step in range(1, n_col):
        col_copy(step, lax.rem(my_col + n_col - step, n_col)).wait_recv()
    pooled_sum = jnp.zeros((8, width), F32)
    shared = []
    for row in range(n_row):
        for col in range(n_col):
            shared.append(table[col, row, :ctx_rows])
            pooled_sum += table[col, row, ctx_rows:]
    pooled = jnp.sum(pooled_sum, axis=0, keepdims=True) / math.sqrt(nodes * n_row * n_col)
    regions = n_row * n_col * ctx_rows
    w_pair = jnp.concatenate([nw1[l, 2 * width :] for l in range(LAYERS)], axis=1)
    projected = mm(jnp.concatenate(shared, axis=0).astype(BF16), w_pair).astype(BF16)
    for line in range(nodes // LANES):
        picker = pick_rows(as_column(region_ref[line : line + 1, :]), regions)
        ctx_part[line * LANES : (line + 1) * LANES, :] = mm(picker, projected)
    shifts = [
        nb[0, l : l + 1]
        + jnp.dot(
            pooled, nwg[l].astype(F32), precision=lax.Precision.HIGHEST, preferred_element_type=F32
        )
        for l in range(LAYERS)
    ]
    node_phase(0, node_ref, shifts[0])

    picked[1] = mm(hot_index[...], node_out[...]).astype(BF16)
    halo_start(1)
    fill_own(1, node_out)
    halo_wait(1)
    edge_phase(1)
    node_phase(1, node_out, shifts[1])

    for layer in range(LAYERS):
        for side in range(4):

            @pl.when(moves[side][2])
            def _(layer=layer, side=side):
                halo_copy(layer, side).wait_send()

    for step in range(1, n_row):
        row_copy(step, my_row).wait_send()
    for step in range(1, n_col):
        col_copy(step, my_col).wait_send()


def local(n_row, n_col, *args):
    node, edge, send, recv, index, ctx, region = args[:7]
    nodes, width = node.shape
    edges = edge.shape[0]
    count = index.shape[2]
    half_ext, half_own = (nodes + 4 * count) // 2, nodes // 2
    vmem = pl.BlockSpec(memory_space=pltpu.VMEM)
    dma = pltpu.SemaphoreType.DMA
    operands = (
        node,
        edge,
        send.reshape(edges // LANES, LANES),
        recv.reshape(edges // LANES, LANES),
        index.reshape(4, count),
        ctx,
        region.reshape(nodes // LANES, LANES),
    ) + args[7:]
    operands = tuple(
        jnp.transpose(x, (1, 0, 2)) if x.shape == (LAYERS, 3, width) else x for x in operands
    )
    return pl.pallas_call(
        functools.partial(kernel, n_row, n_col),
        out_shape=(
            jax.ShapeDtypeStruct(node.shape, BF16),
            jax.ShapeDtypeStruct(edge.shape, BF16),
        ),
        in_specs=[vmem, pl.BlockSpec(memory_space=pl.ANY)] + [vmem] * (len(operands) - 2),
        out_specs=(vmem, vmem),
        scratch_shapes=[
            pltpu.VMEM((edges, half_ext), BF16),
            pltpu.VMEM((edges, half_own), BF16),
            pltpu.VMEM((edges // (2 * BLOCK), half_own, 2 * BLOCK), BF16),
            pltpu.VMEM((edges, width), jnp.int32),
            pltpu.VMEM((edges, width), jnp.int32),
            pltpu.VMEM((4 * count, nodes), BF16),
            pltpu.VMEM((LAYERS, 4 * count, width), BF16),
            pltpu.VMEM((LAYERS, 4 * count, width), BF16),
            pltpu.VMEM((n_col, n_row, ctx.shape[0] + 8, width), F32),
            pltpu.VMEM((half_ext, 2 * width), BF16),
            pltpu.VMEM((half_own, 2 * width), BF16),
            pltpu.VMEM((half_own, 2 * width), F32),
            pltpu.VMEM((nodes, LAYERS * width), F32),
            pltpu.VMEM((2 * BLOCK, 2 * width), BF16),
            dma(()),
            dma((LAYERS, 4)),
            dma((LAYERS, 4)),
            dma((n_row - 1,)),
            dma((n_row - 1,)),
            dma((n_col - 1,)),
            dma((n_col - 1,)),
        ],
        compiler_params=pltpu.CompilerParams(
            collective_id=0, has_side_effects=True, vmem_limit_bytes=36 * 1024 * 1024
        ),
        name="mesh_steps",
    )(*operands)


def solution(mesh):
    both = ("row", "col")
    split = (P(both, None), P(both, None), P(both), P(both), P(both, None, None), P(both, None), P(both))
    return jax.shard_map(
        functools.partial(local, mesh.shape["row"], mesh.shape["col"]),
        mesh=mesh,
        in_specs=split + (P(),) * 9,
        out_specs=(P(both, None), P(both, None)),
        check_vma=False,
    )
```

```python
import functools
import math

import jax
import jax.numpy as jnp
from jax import lax
from jax.experimental import pallas as pl
from jax.experimental.pallas import tpu as pltpu
from jax.sharding import PartitionSpec as P

LAYERS = 2
EPS = 1e-05
LANES = 128
BLOCK = 512
F32 = jnp.float32
BF16 = jnp.bfloat16
MESH = pl.DeviceIdType.MESH


def mm(a, b):
    return jnp.dot(a, b, preferred_element_type=F32)


def iota(axis):
    return lax.broadcasted_iota(jnp.int32, (LANES, LANES), axis)


def as_column(row):
    return jnp.transpose(jnp.broadcast_to(row, (LANES, LANES)))


def hot(mask):
    return jnp.where(mask, 1.0, 0.0).astype(BF16)


def pick_parts(index, axis, count):
    base = hot((index & (LANES - 1)) == iota(axis))
    group = (index >> 7).astype(F32).astype(BF16)
    zero = jnp.zeros_like(base)
    return [
        jnp.where(group == jnp.asarray(part, BF16), base, zero) for part in range(count // LANES)
    ]


def pick_rows(column, count):
    return jnp.concatenate(pick_parts(column, 1, count), axis=1)


def centre(values):
    values = values.astype(F32)
    return values - jnp.mean(values, axis=-1, keepdims=True)


def twice(weight):
    zero = jnp.zeros_like(weight)
    top = jnp.concatenate([weight, zero], axis=1)
    return jnp.concatenate([top, jnp.concatenate([zero, weight], axis=1)], axis=0)


def norm(centred, gain, shift):
    spread = jnp.mean(centred * centred, axis=-1, keepdims=True)
    return centred * lax.rsqrt(spread + EPS) * gain + shift


def kernel(
    n_row,
    n_col,
    rest,
    node_ref,
    edge_ref,
    send_ref,
    recv_ref,
    index_ref,
    ctx_ref,
    region_ref,
    ew1,
    ew2,
    eb,
    eg,
    nw1,
    nwg,
    nw2,
    nb,
    ng,
    node_out,
    edge_out,
    hot_send,
    hot_recv,
    hot_sum,
    side_send,
    side_recv,
    hot_index,
    picked,
    halo,
    table,
    from_ext,
    from_own,
    sums,
    ctx_part,
    parts,
    edge_sem,
    halo_send_sem,
    halo_recv_sem,
    row_send_sem,
    row_recv_sem,
    col_send_sem,
    col_recv_sem,
):
    my_row, my_col = lax.axis_index("row"), lax.axis_index("col")
    nodes, width = node_ref.shape
    edges = edge_ref.shape[0]
    count = index_ref.shape[1]
    ext = nodes + 4 * count
    half_ext, half_own = ext // 2, nodes // 2
    ctx_rows = ctx_ref.shape[0]
    edge_in = pltpu.make_async_copy(edge_ref, edge_out, edge_sem)
    edge_in.start()
    per_block = 2 * BLOCK // LANES

    barrier = pltpu.get_barrier_semaphore()
    for step in range(1, n_row):
        pl.semaphore_signal(
            barrier, inc=1, device_id=(lax.rem(my_row + step, n_row), my_col), device_id_type=MESH
        )
    for step in range(1, n_col):
        pl.semaphore_signal(
            barrier, inc=1, device_id=(my_row, lax.rem(my_col + step, n_col)), device_id_type=MESH
        )

    for side in range(4):
        rows = slice(side * count, (side + 1) * count)
        hot_index[rows, :] = pick_rows(as_column(index_ref[side : side + 1, :]), nodes)
    picked[0] = mm(hot_index[...], node_ref[...]).astype(BF16)
    part = jnp.sum(node_ref[...].astype(F32).reshape(nodes // 8, 8, width), axis=0)
    table[my_col, my_row] = jnp.concatenate([ctx_ref[...].astype(F32), part], axis=0)

    pl.semaphore_wait(barrier, n_row + n_col - 2)

    moves = (
        (my_row + 1, my_col, my_row < n_row - 1, my_row > 0),
        (my_row - 1, my_col, my_row > 0, my_row < n_row - 1),
        (my_row, my_col + 1, my_col < n_col - 1, my_col > 0),
        (my_row, my_col - 1, my_col > 0, my_col < n_col - 1),
    )

    def halo_copy(layer, side):
        to_row, to_col = moves[side][:2]
        rows = pl.ds(side * count, count)
        return pltpu.make_async_remote_copy(
            src_ref=picked.at[layer, rows],
            dst_ref=halo.at[layer, rows],
            send_sem=halo_send_sem.at[layer, side],
            recv_sem=halo_recv_sem.at[layer, side],
            device_id=(to_row, to_col),
            device_id_type=MESH,
        )

    def halo_start(layer):
        for side in range(4):

            @pl.when(moves[side][2])
            def _(side=side):
                halo_copy(layer, side).start()

    def halo_wait(layer):
        for side in range(4):

            @pl.when(moves[side][3])
            def _(side=side):
                halo_copy(layer, side).wait_recv()

            @pl.when(jnp.logical_not(moves[side][3]))
            def _(side=side):
                halo[layer, side * count : (side + 1) * count] = jnp.zeros((count, width), BF16)

    def row_copy(step, owner):
        return pltpu.make_async_remote_copy(
            src_ref=table.at[my_col, owner],
            dst_ref=table.at[my_col, owner],
            send_sem=row_send_sem.at[step - 1],
            recv_sem=row_recv_sem.at[step - 1],
            device_id=(lax.rem(my_row + step, n_row), my_col),
            device_id_type=MESH,
        )

    def col_copy(step, owner):
        return pltpu.make_async_remote_copy(
            src_ref=table.at[owner],
            dst_ref=table.at[owner],
            send_sem=col_send_sem.at[step - 1],
            recv_sem=col_recv_sem.at[step - 1],
            device_id=(my_row, lax.rem(my_col + step, n_col)),
            device_id_type=MESH,
        )

    halo_start(0)
    for step in range(1, n_row):
        row_copy(step, my_row).start()
    for copy in rest:
        copy.wait()

    def prepare(block, carry):
        for sub in range(per_block):
            line = block * per_block + sub
            send_row = send_ref[pl.ds(line, 1), :]
            recv_row = recv_ref[pl.ds(line, 1), :]
            rows = pl.ds(pl.multiple_of(line * LANES, LANES), LANES)
            both = as_column(send_row + (recv_row << 16))
            send, recv = both & 0xFFFF, both >> 16
            send_high = (send >= half_ext).astype(jnp.int32)
            side_send[rows, :] = send_high
            recv_high = (recv >= half_own).astype(jnp.int32)
            side_recv[rows, :] = recv_high
            hot_send[rows, :] = pick_rows(send - send_high * half_ext, half_ext)
            hot_recv[rows, :] = pick_rows(recv - recv_high * half_own, half_own)
            recv_low = recv_row - (recv_row >= half_own).astype(jnp.int32) * half_own
            recv_low = jnp.broadcast_to(recv_low, (LANES, LANES))
            for part, value in enumerate(pick_parts(recv_low, 0, half_own)):
                hot_sum[
                    block, part * LANES : (part + 1) * LANES, sub * LANES : (sub + 1) * LANES
                ] = value
        return carry

    lax.fori_loop(0, edges // (2 * BLOCK), prepare, 0)

    for step in range(1, n_row):
        row_copy(step, lax.rem(my_row + n_row - step, n_row)).wait_recv()
    for step in range(1, n_col):
        col_copy(step, my_col).start()

    def fill_own(layer, now):
        w_pair = jnp.concatenate([ew1[layer, :width], ew1[layer, width : 2 * width]], axis=1)
        both = mm(now[...], w_pair).astype(BF16)
        from_ext[:, :width] = both[:half_ext, :width]
        from_ext[: nodes - half_ext, width:] = both[half_ext:, :width]
        from_own[:, :width] = both[:half_own, width:]
        from_own[:, width:] = both[half_own:, width:]

    def edge_phase(layer):
        from_ext[nodes - half_ext :, width:] = mm(halo[layer], ew1[layer, :width]).astype(BF16)
        sums[...] = jnp.zeros_like(sums)
        parts[...] = jnp.zeros_like(parts)
        w_edge = twice(ew1[layer, 2 * width :])
        w_out = twice(centre(ew2[layer]).astype(BF16))
        b_in = eb[0, layer : layer + 1]
        b_out = centre(eb[1, layer : layer + 1])

        def scatter(pair):
            sums[...] += mm(hot_sum[pair], parts[...])

        def body(pair, carry):
            blocks = [
                pl.ds(pl.multiple_of((2 * pair + half) * BLOCK, BLOCK), BLOCK) for half in range(2)
            ]
            old = [edge_out[rows, :] for rows in blocks]
            by_edge = mm(jnp.concatenate(old, axis=1), w_edge)
            by_send = [mm(hot_send[rows, :], from_ext[...]) for rows in blocks]
            by_recv = [mm(hot_recv[rows, :], from_own[...]) for rows in blocks]
            scatter(jnp.maximum(pair - 1, 0))
            hidden = []
            for half, rows in enumerate(blocks):
                pre = by_edge[:, half * width : (half + 1) * width] + b_in
                pre += jnp.where(
                    side_send[rows, :] > 0, by_send[half][:, width:], by_send[half][:, :width]
                )
                pre += jnp.where(
                    side_recv[rows, :] > 0, by_recv[half][:, width:], by_recv[half][:, :width]
                )
                hidden.append(jnp.maximum(pre, 0.0).astype(BF16))
            y_val = mm(jnp.concatenate(hidden, axis=1), w_out)
            for half, rows in enumerate(blocks):
                centred = y_val[:, half * width : (half + 1) * width] + b_out
                new = old[half].astype(F32)
                new += norm(centred, eg[layer : layer + 1], eb[2, layer : layer + 1])
                edge_out[rows, :] = new.astype(BF16)
                high = side_recv[rows, :] > 0
                place = slice(half * BLOCK, (half + 1) * BLOCK)
                parts[place, :width] = jnp.where(high, 0.0, new).astype(BF16)
                parts[place, width:] = jnp.where(high, new, 0.0).astype(BF16)
            return carry

        pairs = edges // (2 * BLOCK)
        lax.fori_loop(0, pairs, body, 0)
        scatter(pairs - 1)

    def node_phase(layer, now, shift_in):
        summed = jnp.concatenate([sums[:, :width], sums[:, width:]], axis=0).astype(BF16)
        feats = jnp.concatenate([now[...], summed], axis=1)
        pre = mm(feats, nw1[layer, : 2 * width]) + shift_in
        pre += ctx_part[:, layer * width : (layer + 1) * width]
        hidden = jnp.maximum(pre, 0.0).astype(BF16)
        centred = mm(hidden, centre(nw2[layer]).astype(BF16)) + centre(nb[1, layer : layer + 1])
        new = now[...].astype(F32)
        new += norm(centred, ng[layer : layer + 1], nb[2, layer : layer + 1])
        node_out[...] = new.astype(BF16)

    fill_own(0, node_ref)
    halo_wait(0)
    edge_in.wait()
    edge_phase(0)

    for step in range(1, n_col):
        col_copy(step, lax.rem(my_col + n_col - step, n_col)).wait_recv()
    pooled_sum = jnp.zeros((8, width), F32)
    shared = []
    for row in range(n_row):
        for col in range(n_col):
            shared.append(table[col, row, :ctx_rows])
            pooled_sum += table[col, row, ctx_rows:]
    pooled = jnp.sum(pooled_sum, axis=0, keepdims=True) / math.sqrt(nodes * n_row * n_col)
    regions = n_row * n_col * ctx_rows
    w_pair = jnp.concatenate([nw1[l, 2 * width :] for l in range(LAYERS)], axis=1)
    projected = mm(jnp.concatenate(shared, axis=0).astype(BF16), w_pair).astype(BF16)
    for line in range(nodes // LANES):
        picker = pick_rows(as_column(region_ref[line : line + 1, :]), regions)
        ctx_part[line * LANES : (line + 1) * LANES, :] = mm(picker, projected)
    shifts = [
        nb[0, l : l + 1]
        + jnp.dot(
            pooled, nwg[l].astype(F32), precision=lax.Precision.HIGHEST, preferred_element_type=F32
        )
        for l in range(LAYERS)
    ]
    node_phase(0, node_ref, shifts[0])

    picked[1] = mm(hot_index[...], node_out[...]).astype(BF16)
    halo_start(1)
    fill_own(1, node_out)
    halo_wait(1)
    edge_phase(1)
    node_phase(1, node_out, shifts[1])

    for layer in range(LAYERS):
        for side in range(4):

            @pl.when(moves[side][2])
            def _(layer=layer, side=side):
                halo_copy(layer, side).wait_send()

    for step in range(1, n_row):
        row_copy(step, my_row).wait_send()
    for step in range(1, n_col):
        col_copy(step, my_col).wait_send()


EARLY = (0, 4, 5)


def entry(n_row, n_col, count, *refs):
    given, others = refs[:count], list(refs[count : -count])
    held, copy_sem = refs[-count:-1], refs[-1]
    places = list(held)
    places.insert(1, None)
    copies = {
        k: pltpu.make_async_copy(given[k], places[k], copy_sem.at[k])
        for k in range(count)
        if k != 1
    }
    order = EARLY + tuple(k for k in copies if k not in EARLY)
    for k in order:
        copies[k].start()
    for k in EARLY:
        copies[k].wait()
    places[1] = given[1]
    rest = [copies[k] for k in order if k not in EARLY]
    kernel(n_row, n_col, rest, *places, *others)


def local(n_row, n_col, *args):
    node, edge, send, recv, index, ctx, region = args[:7]
    nodes, width = node.shape
    edges = edge.shape[0]
    count = index.shape[2]
    half_ext, half_own = (nodes + 4 * count) // 2, nodes // 2
    vmem = pl.BlockSpec(memory_space=pltpu.VMEM)
    dma = pltpu.SemaphoreType.DMA
    operands = (
        node,
        edge,
        send.reshape(edges // LANES, LANES),
        recv.reshape(edges // LANES, LANES),
        index.reshape(4, count),
        ctx,
        region.reshape(nodes // LANES, LANES),
    ) + args[7:]
    operands = tuple(
        jnp.transpose(x, (1, 0, 2)) if x.shape == (LAYERS, 3, width) else x for x in operands
    )
    operands = tuple(pltpu.with_memory_space_constraint(x, pltpu.HBM) for x in operands)
    return pl.pallas_call(
        functools.partial(entry, n_row, n_col, len(operands)),
        out_shape=(
            jax.ShapeDtypeStruct(node.shape, BF16),
            jax.ShapeDtypeStruct(edge.shape, BF16),
        ),
        in_specs=[pl.BlockSpec(memory_space=pltpu.HBM)] * len(operands),
        out_specs=(vmem, vmem),
        scratch_shapes=[
            pltpu.VMEM((edges, half_ext), BF16),
            pltpu.VMEM((edges, half_own), BF16),
            pltpu.VMEM((edges // (2 * BLOCK), half_own, 2 * BLOCK), BF16),
            pltpu.VMEM((edges, width), jnp.int32),
            pltpu.VMEM((edges, width), jnp.int32),
            pltpu.VMEM((4 * count, nodes), BF16),
            pltpu.VMEM((LAYERS, 4 * count, width), BF16),
            pltpu.VMEM((LAYERS, 4 * count, width), BF16),
            pltpu.VMEM((n_col, n_row, ctx.shape[0] + 8, width), F32),
            pltpu.VMEM((half_ext, 2 * width), BF16),
            pltpu.VMEM((half_own, 2 * width), BF16),
            pltpu.VMEM((half_own, 2 * width), F32),
            pltpu.VMEM((nodes, LAYERS * width), F32),
            pltpu.VMEM((2 * BLOCK, 2 * width), BF16),
            dma(()),
            dma((LAYERS, 4)),
            dma((LAYERS, 4)),
            dma((n_row - 1,)),
            dma((n_row - 1,)),
            dma((n_col - 1,)),
            dma((n_col - 1,)),
        ]
        + [pltpu.VMEM(x.shape, x.dtype) for k, x in enumerate(operands) if k != 1]
        + [dma((len(operands),))],
        compiler_params=pltpu.CompilerParams(
            collective_id=0, has_side_effects=True, vmem_limit_bytes=36 * 1024 * 1024
        ),
        name="mesh_steps",
    )(*operands)


def solution(mesh):
    both = ("row", "col")
    split = (P(both, None), P(both, None), P(both), P(both), P(both, None, None), P(both, None), P(both))
    return jax.shard_map(
        functools.partial(local, mesh.shape["row"], mesh.shape["col"]),
        mesh=mesh,
        in_specs=split + (P(),) * 9,
        out_specs=(P(both, None), P(both, None)),
        check_vma=False,
    )
```

```python
import functools
import math

import jax
import jax.numpy as jnp
from jax import lax
from jax.experimental import pallas as pl
from jax.experimental.pallas import tpu as pltpu
from jax.sharding import PartitionSpec as P

LAYERS = 2
EPS = 1e-05
LANES = 128
BLOCK = 512
F32 = jnp.float32
BF16 = jnp.bfloat16
MESH = pl.DeviceIdType.MESH


def mm(a, b):
    return jnp.dot(a, b, preferred_element_type=F32)


def iota(axis):
    return lax.broadcasted_iota(jnp.int32, (LANES, LANES), axis)


def as_column(row):
    return jnp.transpose(jnp.broadcast_to(row, (LANES, LANES)))


def hot(mask):
    return jnp.where(mask, 1.0, 0.0).astype(BF16)


def pick_parts(index, axis, count):
    base = hot((index & (LANES - 1)) == iota(axis))
    group = (index >> 7).astype(F32).astype(BF16)
    zero = jnp.zeros_like(base)
    return [
        jnp.where(group == jnp.asarray(part, BF16), base, zero) for part in range(count // LANES)
    ]


def pick_rows(column, count):
    return jnp.concatenate(pick_parts(column, 1, count), axis=1)


def centre(values):
    values = values.astype(F32)
    return values - jnp.mean(values, axis=-1, keepdims=True)


def twice(weight):
    zero = jnp.zeros_like(weight)
    top = jnp.concatenate([weight, zero], axis=1)
    return jnp.concatenate([top, jnp.concatenate([zero, weight], axis=1)], axis=0)


def norm(centred, gain, shift):
    spread = jnp.mean(centred * centred, axis=-1, keepdims=True)
    return centred * lax.rsqrt(spread + EPS) * gain + shift


def kernel(
    n_row,
    n_col,
    rest,
    node_ref,
    edge_ref,
    send_ref,
    recv_ref,
    index_ref,
    ctx_ref,
    region_ref,
    ew1,
    ew2,
    eb,
    eg,
    nw1,
    nwg,
    nw2,
    nb,
    ng,
    node_out,
    edge_out,
    hot_send,
    hot_recv,
    hot_sum,
    side_send,
    side_recv,
    hot_index,
    picked,
    halo,
    table,
    from_ext,
    from_own,
    sums,
    ctx_part,
    parts,
    edge_sem,
    halo_send_sem,
    halo_recv_sem,
    row_send_sem,
    row_recv_sem,
    col_send_sem,
    col_recv_sem,
):
    my_row, my_col = lax.axis_index("row"), lax.axis_index("col")
    nodes, width = node_ref.shape
    edges = edge_ref.shape[0]
    count = index_ref.shape[1]
    ext = nodes + 4 * count
    half_ext, half_own = ext // 2, nodes // 2
    ctx_rows = ctx_ref.shape[0]
    edge_in = pltpu.make_async_copy(edge_ref, edge_out, edge_sem)
    edge_in.start()
    per_block = 2 * BLOCK // LANES

    barrier = pltpu.get_barrier_semaphore()
    for step in range(1, n_row):
        pl.semaphore_signal(
            barrier, inc=1, device_id=(lax.rem(my_row + step, n_row), my_col), device_id_type=MESH
        )
    for step in range(1, n_col):
        pl.semaphore_signal(
            barrier, inc=1, device_id=(my_row, lax.rem(my_col + step, n_col)), device_id_type=MESH
        )

    for side in range(4):
        rows = slice(side * count, (side + 1) * count)
        hot_index[rows, :] = pick_rows(as_column(index_ref[side : side + 1, :]), nodes)
    picked[0] = mm(hot_index[...], node_ref[...]).astype(BF16)
    part = jnp.sum(node_ref[...].astype(F32).reshape(nodes // 8, 8, width), axis=0)
    table[my_col, my_row] = jnp.concatenate([ctx_ref[...].astype(F32), part], axis=0)

    pl.semaphore_wait(barrier, n_row + n_col - 2)

    moves = (
        (my_row + 1, my_col, my_row < n_row - 1, my_row > 0),
        (my_row - 1, my_col, my_row > 0, my_row < n_row - 1),
        (my_row, my_col + 1, my_col < n_col - 1, my_col > 0),
        (my_row, my_col - 1, my_col > 0, my_col < n_col - 1),
    )

    def halo_copy(layer, side):
        to_row, to_col = moves[side][:2]
        rows = pl.ds(side * count, count)
        return pltpu.make_async_remote_copy(
            src_ref=picked.at[layer, rows],
            dst_ref=halo.at[layer, rows],
            send_sem=halo_send_sem.at[layer, side],
            recv_sem=halo_recv_sem.at[layer, side],
            device_id=(to_row, to_col),
            device_id_type=MESH,
        )

    def halo_start(layer):
        for side in range(4):

            @pl.when(moves[side][2])
            def _(side=side):
                halo_copy(layer, side).start()

    def halo_wait(layer):
        for side in range(4):

            @pl.when(moves[side][3])
            def _(side=side):
                halo_copy(layer, side).wait_recv()

            @pl.when(jnp.logical_not(moves[side][3]))
            def _(side=side):
                halo[layer, side * count : (side + 1) * count] = jnp.zeros((count, width), BF16)

    def row_copy(step, owner):
        return pltpu.make_async_remote_copy(
            src_ref=table.at[my_col, owner],
            dst_ref=table.at[my_col, owner],
            send_sem=row_send_sem.at[step - 1],
            recv_sem=row_recv_sem.at[step - 1],
            device_id=(lax.rem(my_row + step, n_row), my_col),
            device_id_type=MESH,
        )

    def col_copy(step, owner):
        return pltpu.make_async_remote_copy(
            src_ref=table.at[owner],
            dst_ref=table.at[owner],
            send_sem=col_send_sem.at[step - 1],
            recv_sem=col_recv_sem.at[step - 1],
            device_id=(my_row, lax.rem(my_col + step, n_col)),
            device_id_type=MESH,
        )

    halo_start(0)
    for step in range(1, n_row):
        row_copy(step, my_row).start()
    for copy in rest:
        copy.wait()

    def prepare(block, carry):
        for sub in range(per_block):
            line = block * per_block + sub
            send_row = send_ref[pl.ds(line, 1), :]
            recv_row = recv_ref[pl.ds(line, 1), :]
            rows = pl.ds(pl.multiple_of(line * LANES, LANES), LANES)
            both = as_column(send_row + (recv_row << 16))
            send, recv = both & 0xFFFF, both >> 16
            send_high = (send >= half_ext).astype(jnp.int32)
            side_send[rows, :] = send_high
            recv_high = (recv >= half_own).astype(jnp.int32)
            side_recv[rows, :] = recv_high
            hot_send[rows, :] = pick_rows(send - send_high * half_ext, half_ext)
            hot_recv[rows, :] = pick_rows(recv - recv_high * half_own, half_own)
            recv_low = recv_row - (recv_row >= half_own).astype(jnp.int32) * half_own
            recv_low = jnp.broadcast_to(recv_low, (LANES, LANES))
            for part, value in enumerate(pick_parts(recv_low, 0, half_own)):
                hot_sum[
                    block, part * LANES : (part + 1) * LANES, sub * LANES : (sub + 1) * LANES
                ] = value
        return carry

    lax.fori_loop(0, edges // (2 * BLOCK), prepare, 0)

    for step in range(1, n_row):
        row_copy(step, lax.rem(my_row + n_row - step, n_row)).wait_recv()
    for step in range(1, n_col):
        col_copy(step, my_col).start()

    def fill_own(layer, now):
        w_pair = jnp.concatenate([ew1[layer, :width], ew1[layer, width : 2 * width]], axis=1)
        both = mm(now[...], w_pair).astype(BF16)
        from_ext[:, :width] = both[:half_ext, :width]
        from_ext[: nodes - half_ext, width:] = both[half_ext:, :width]
        from_own[:, :width] = both[:half_own, width:]
        from_own[:, width:] = both[half_own:, width:]

    def edge_phase(layer):
        from_ext[nodes - half_ext :, width:] = mm(halo[layer], ew1[layer, :width]).astype(BF16)
        sums[...] = jnp.zeros_like(sums)
        parts[...] = jnp.zeros_like(parts)
        w_edge = twice(ew1[layer, 2 * width :])
        w_out = twice(centre(ew2[layer]).astype(BF16))
        b_in = eb[0, layer : layer + 1]
        b_out = centre(eb[1, layer : layer + 1])

        def scatter(pair):
            sums[...] += mm(hot_sum[pair], parts[...])

        def body(pair, carry):
            blocks = [
                pl.ds(pl.multiple_of((2 * pair + half) * BLOCK, BLOCK), BLOCK) for half in range(2)
            ]
            old = [edge_out[rows, :] for rows in blocks]
            by_edge = mm(jnp.concatenate(old, axis=1), w_edge)
            by_send = [mm(hot_send[rows, :], from_ext[...]) for rows in blocks]
            by_recv = [mm(hot_recv[rows, :], from_own[...]) for rows in blocks]
            scatter(jnp.maximum(pair - 1, 0))
            hidden = []
            for half, rows in enumerate(blocks):
                pre = by_edge[:, half * width : (half + 1) * width] + b_in
                pre += jnp.where(
                    side_send[rows, :] > 0, by_send[half][:, width:], by_send[half][:, :width]
                )
                pre += jnp.where(
                    side_recv[rows, :] > 0, by_recv[half][:, width:], by_recv[half][:, :width]
                )
                hidden.append(jnp.maximum(pre, 0.0).astype(BF16))
            y_val = mm(jnp.concatenate(hidden, axis=1), w_out)
            for half, rows in enumerate(blocks):
                centred = y_val[:, half * width : (half + 1) * width] + b_out
                new = old[half].astype(F32)
                new += norm(centred, eg[layer : layer + 1], eb[2, layer : layer + 1])
                edge_out[rows, :] = new.astype(BF16)
                high = side_recv[rows, :] > 0
                place = slice(half * BLOCK, (half + 1) * BLOCK)
                parts[place, :width] = jnp.where(high, 0.0, new).astype(BF16)
                parts[place, width:] = jnp.where(high, new, 0.0).astype(BF16)
            return carry

        pairs = edges // (2 * BLOCK)
        lax.fori_loop(0, pairs, body, 0)
        scatter(pairs - 1)

    def node_phase(layer, now, shift_in):
        summed = jnp.concatenate([sums[:, :width], sums[:, width:]], axis=0).astype(BF16)
        feats = jnp.concatenate([now[...], summed], axis=1)
        pre = mm(feats, nw1[layer, : 2 * width]) + shift_in
        pre += ctx_part[:, layer * width : (layer + 1) * width]
        hidden = jnp.maximum(pre, 0.0).astype(BF16)
        centred = mm(hidden, centre(nw2[layer]).astype(BF16)) + centre(nb[1, layer : layer + 1])
        new = now[...].astype(F32)
        new += norm(centred, ng[layer : layer + 1], nb[2, layer : layer + 1])
        node_out[...] = new.astype(BF16)

    fill_own(0, node_ref)
    halo_wait(0)
    edge_in.wait()
    edge_phase(0)

    for step in range(1, n_col):
        col_copy(step, lax.rem(my_col + n_col - step, n_col)).wait_recv()
    pooled_sum = jnp.zeros((8, width), F32)
    shared = []
    for row in range(n_row):
        for col in range(n_col):
            shared.append(table[col, row, :ctx_rows])
            pooled_sum += table[col, row, ctx_rows:]
    pooled = jnp.sum(pooled_sum, axis=0, keepdims=True) / math.sqrt(nodes * n_row * n_col)
    regions = n_row * n_col * ctx_rows
    w_pair = jnp.concatenate([nw1[l, 2 * width :] for l in range(LAYERS)], axis=1)
    projected = mm(jnp.concatenate(shared, axis=0).astype(BF16), w_pair).astype(BF16)
    for line in range(nodes // LANES):
        picker = pick_rows(as_column(region_ref[line : line + 1, :]), regions)
        ctx_part[line * LANES : (line + 1) * LANES, :] = mm(picker, projected)
    def shift_of(layer):
        weight = nwg[layer].astype(F32)
        term = jnp.dot(
            pooled, weight, precision=lax.Precision.HIGHEST, preferred_element_type=F32
        )
        return nb[0, layer : layer + 1] + term

    node_phase(0, node_ref, shift_of(0))

    picked[1] = mm(hot_index[...], node_out[...]).astype(BF16)
    halo_start(1)
    fill_own(1, node_out)
    last_shift = shift_of(1)
    halo_wait(1)
    edge_phase(1)
    node_phase(1, node_out, last_shift)

    for layer in range(LAYERS):
        for side in range(4):

            @pl.when(moves[side][2])
            def _(layer=layer, side=side):
                halo_copy(layer, side).wait_send()

    for step in range(1, n_row):
        row_copy(step, my_row).wait_send()
    for step in range(1, n_col):
        col_copy(step, my_col).wait_send()


EARLY = (0, 4, 5)


def entry(n_row, n_col, count, *refs):
    given, others = refs[:count], list(refs[count : -count])
    held, copy_sem = refs[-count:-1], refs[-1]
    places = list(held)
    places.insert(1, None)
    copies = {
        k: pltpu.make_async_copy(given[k], places[k], copy_sem.at[k])
        for k in range(count)
        if k != 1
    }
    order = EARLY + tuple(k for k in copies if k not in EARLY)
    for k in order:
        copies[k].start()
    for k in EARLY:
        copies[k].wait()
    places[1] = given[1]
    rest = [copies[k] for k in order if k not in EARLY]
    kernel(n_row, n_col, rest, *places, *others)


def local(n_row, n_col, *args):
    node, edge, send, recv, index, ctx, region = args[:7]
    nodes, width = node.shape
    edges = edge.shape[0]
    count = index.shape[2]
    half_ext, half_own = (nodes + 4 * count) // 2, nodes // 2
    vmem = pl.BlockSpec(memory_space=pltpu.VMEM)
    dma = pltpu.SemaphoreType.DMA
    operands = (
        node,
        edge,
        send.reshape(edges // LANES, LANES),
        recv.reshape(edges // LANES, LANES),
        index.reshape(4, count),
        ctx,
        region.reshape(nodes // LANES, LANES),
    ) + args[7:]
    operands = tuple(
        jnp.transpose(x, (1, 0, 2)) if x.shape == (LAYERS, 3, width) else x for x in operands
    )
    operands = tuple(pltpu.with_memory_space_constraint(x, pltpu.HBM) for x in operands)
    return pl.pallas_call(
        functools.partial(entry, n_row, n_col, len(operands)),
        out_shape=(
            jax.ShapeDtypeStruct(node.shape, BF16),
            jax.ShapeDtypeStruct(edge.shape, BF16),
        ),
        in_specs=[pl.BlockSpec(memory_space=pltpu.HBM)] * len(operands),
        out_specs=(vmem, vmem),
        scratch_shapes=[
            pltpu.VMEM((edges, half_ext), BF16),
            pltpu.VMEM((edges, half_own), BF16),
            pltpu.VMEM((edges // (2 * BLOCK), half_own, 2 * BLOCK), BF16),
            pltpu.VMEM((edges, width), jnp.int32),
            pltpu.VMEM((edges, width), jnp.int32),
            pltpu.VMEM((4 * count, nodes), BF16),
            pltpu.VMEM((LAYERS, 4 * count, width), BF16),
            pltpu.VMEM((LAYERS, 4 * count, width), BF16),
            pltpu.VMEM((n_col, n_row, ctx.shape[0] + 8, width), F32),
            pltpu.VMEM((half_ext, 2 * width), BF16),
            pltpu.VMEM((half_own, 2 * width), BF16),
            pltpu.VMEM((half_own, 2 * width), F32),
            pltpu.VMEM((nodes, LAYERS * width), F32),
            pltpu.VMEM((2 * BLOCK, 2 * width), BF16),
            dma(()),
            dma((LAYERS, 4)),
            dma((LAYERS, 4)),
            dma((n_row - 1,)),
            dma((n_row - 1,)),
            dma((n_col - 1,)),
            dma((n_col - 1,)),
        ]
        + [pltpu.VMEM(x.shape, x.dtype) for k, x in enumerate(operands) if k != 1]
        + [dma((len(operands),))],
        compiler_params=pltpu.CompilerParams(
            collective_id=0, has_side_effects=True, vmem_limit_bytes=36 * 1024 * 1024
        ),
        name="mesh_steps",
    )(*operands)


def solution(mesh):
    both = ("row", "col")
    split = (P(both, None), P(both, None), P(both), P(both), P(both, None, None), P(both, None), P(both))
    return jax.shard_map(
        functools.partial(local, mesh.shape["row"], mesh.shape["col"]),
        mesh=mesh,
        in_specs=split + (P(),) * 9,
        out_specs=(P(both, None), P(both, None)),
        check_vma=False,
    )
```
